128 devices in a mesh: row: 16 (over z, y_lo, core), col: 8 (over x, y_hi).
Axes of the slice: x: 4, y: 4 (y_hi: 2, y_lo: 2; y = y_hi * 2 + y_lo), z: 4, core: 2. Of those that a mesh axis runs over, the one named last changes fastest.
Arguments:
- hamiltonian: float32 [8192, 8192], P(('row', 'col')), may hold values from -0.0625 to 0.0625
- coefficients: float32 [8192, 4096], P('row', 'col'), may hold values from -6 to 6
Outputs:
- applied: float32 [8192, 4096], P('row', 'col')
The draws below stay inside these ranges and needn't reach their ends.
All inputs are finite; a program needn't handle non-finite values.
Results may differ from the reference program's by a relative error of at most 0.00007.
Values sent between devices are 32-bit elements; how exact they have to be, the bound alone decides.
A program may use at most 128 MiB of HBM per device.

```python
import jax
import jax.numpy as jnp
from jax import lax

M = 8192
NORB = 4096


def levels(stream_key, extent, pieces, low, top_value):
    factor_of, own = 1.0, jax.random.fold_in(stream_key, 6)
    for axis_at, parts in pieces:
        heights = jnp.exp(jax.random.uniform(jax.random.fold_in(own, axis_at), (parts,), jnp.float32, low / len(pieces), top_value / len(pieces)))
        factor_of = factor_of * jnp.repeat(heights, extent[axis_at] // parts).reshape([-1 if axis == axis_at else 1 for axis in range(len(extent))])
    return factor_of


def scatter_about(stream_key, extent, spread, most, shards=(), kind=jnp.bfloat16):
    factor_of = levels(stream_key, extent, shards, -0.22, 0.18) if shards else 1.0
    drawn = jax.random.normal(stream_key, extent, jnp.float32) * spread * factor_of
    return jnp.minimum(jnp.maximum(drawn, -most), most).astype(kind)


def setup_inputs(seed: int = 0) -> dict:
    streams_of = jax.random.split(jax.random.key(seed), 3)
    hamiltonian = scatter_about(streams_of[0], (M, M), M ** -0.5, 0.0625, ((0, 128),), jnp.float32)
    coefficients = scatter_about(streams_of[1], (M, NORB), 1.0, 6.0, ((0, 16), (1, 8)), jnp.float32)
    return dict(hamiltonian=hamiltonian, coefficients=coefficients)


def reference(hamiltonian, coefficients):
    return jnp.dot(hamiltonian, coefficients, precision=lax.Precision.HIGHEST, preferred_element_type=jnp.float32)
```

```python
import jax
import jax.numpy as jnp
from jax import lax
from jax.experimental import pallas as pl
from jax.experimental.pallas import tpu as pltpu
from jax.sharding import PartitionSpec as P

MESH = pl.DeviceIdType.MESH
F32, BF16 = jnp.float32, jnp.bfloat16
SUB = 64
DEEP = 2048
WIDE = 512
SLOT = {2: 0, 1: 1, 3: 2, 0: 3}


def kernel(h_ref, c_ref, o_ref, hb, rl, cb, c3, h3, h2, hs, part, parts, r0, r13, r2, ssem, rsem, lsem):
    row, col = lax.axis_index("row"), lax.axis_index("col")
    z, yl, core = lax.div(row, 4), lax.rem(lax.div(row, 2), 2), lax.rem(row, 2)
    x, yh = lax.div(col, 2), lax.rem(col, 2)

    def device(z=z, yl=yl, core=core, x=x, yh=yh):
        return ((z * 2 + yl) * 2 + core, x * 2 + yh)

    def up(v, d):
        return lax.rem(v + d, 4)

    zp, zm = device(z=up(z, 1)), device(z=up(z, 3))
    xp, xm = device(x=up(x, 1)), device(x=up(x, 3))
    ya, yb, yc = device(yl=1 - yl), device(yl=1 - yl, yh=1 - yh), device(yh=1 - yh)
    twin = device(core=1 - core)

    barrier = pltpu.get_barrier_semaphore()
    for other in (zp, zm, xp, xm, ya, yb, yc, twin):
        pl.semaphore_signal(barrier, inc=1, device_id=other, device_id_type=MESH)
    pl.semaphore_wait(barrier, 8)

    sent, local = [], []

    def send(src, dst, to):
        n = len(sent)
        copy = pltpu.make_async_remote_copy(
            src_ref=src, dst_ref=dst, send_sem=ssem.at[n], recv_sem=rsem.at[n], device_id=to, device_id_type=MESH
        )
        copy.start()
        sent.append(copy)
        return copy

    def move(src, dst):
        copy = pltpu.make_async_copy(src, dst, lsem.at[len(local)])
        copy.start()
        local.append(copy)
        return copy

    def inner(d):
        return pl.ds(pl.multiple_of(up(z, d) * DEEP, DEEP), DEEP)

    A, B, ALL = pl.ds(0, 32), pl.ds(32, 32), pl.ds(0, 64)
    C0, C1 = pl.ds(0, 256), pl.ds(256, 256)

    to_p, to_m = {}, {}
    own_h = move(h_ref.at[:, inner(0)], hb.at[0, 0])
    own_c = move(c_ref, cb.at[0, core])
    to_p["A"] = send(h_ref.at[A, inner(1)], hb.at[0, 3, A], zp)
    to_m["A"] = send(h_ref.at[A, inner(3)], hb.at[0, 1, A], zm)
    p0, m0, p1, m1 = pl.ds(0, 48), pl.ds(16, 48), pl.ds(48, 16), pl.ds(0, 16)
    x0 = [send(h_ref.at[p0, inner(0)], hb.at[3, 0, p0], xp), send(h_ref.at[m0, inner(0)], hb.at[1, 0, m0], xm)]
    ca1 = send(c_ref.at[C1], cb.at[1, core, C1], ya)
    cb0 = send(c_ref.at[C0], cb.at[2, core, C0], yb)
    to_p["R"] = send(h_ref.at[A, inner(2)], rl.at[0], zp)
    to_m["R"] = send(h_ref.at[B, inner(2)], rl.at[1], zm)
    ca0 = send(c_ref.at[C0], cb.at[1, core, C0], ya)
    cb1 = send(c_ref.at[C1], cb.at[2, core, C1], yb)
    to_p["B"] = send(h_ref.at[B, inner(1)], hb.at[0, 3, B], zp)
    to_m["B"] = send(h_ref.at[B, inner(3)], hb.at[0, 1, B], zm)
    twins = {(0, 0): send(c_ref, cb.at[0, core], twin)}

    def split(src, rows, stores):
        def body(i, _):
            at = pl.multiple_of(i * 16, 16)
            v = src[pl.ds(at, 16), :]
            hi = v.astype(BF16)
            lo = (v - hi.astype(F32)).astype(BF16)
            for store in stores:
                store(at, hi, lo)
            return 0

        lax.fori_loop(0, rows // 16, body, 0)

    def split_h(dx, dz, batch, start, first=0, rows=SUB):
        def store(at, hi, lo):
            to = pl.ds(pl.multiple_of(start + at, 16), 16)
            h3[batch, to, pl.ds(0, DEEP)] = hi
            h3[batch, to, pl.ds(DEEP, DEEP)] = lo
            h3[batch, to, pl.ds(2 * DEEP, DEEP)] = hi

        split(hb.at[dx, dz, pl.ds(first, rows)], rows, [store])

    def stack_h(dx, dz, to, start, height, first=0, rows=SUB):
        def store(at, hi, lo):
            to[pl.ds(pl.multiple_of(start + at, 16), 16), :] = hi
            to[pl.ds(pl.multiple_of(start + height + at, 16), 16), :] = lo

        split(hb.at[dx, dz, pl.ds(first, rows)], rows, [store])

    def split_c(rel, which):
        half = 0 if rel < 2 else 1
        lower = yl if rel in (0, 3) else 1 - yl
        start = lower * 1024 + which * 512

        def store(at, hi, lo):
            to = pl.multiple_of(start + at, 16)
            c3[half, pl.ds(to, 16), :] = hi
            c3[half, pl.ds(to + DEEP, 16), :] = hi
            c3[half, pl.ds(to + 2 * DEEP, 16), :] = lo

        split(cb.at[rel, which], 512, [store])

    def multiply(batch, half, start, rows):
        def body(n, _):
            at = pl.ds(pl.multiple_of(n * 256, 256), 256)
            part[batch, half, pl.ds(start, rows), at] = jnp.dot(
                h3[batch, pl.ds(start, rows), :], c3[half, :, at], preferred_element_type=F32
            )
            return 0

        lax.fori_loop(0, 2, body, 0)

    def multiply_stack(to, stack, half):
        rows = to.shape[0]

        def body(n, _):
            at = pl.ds(pl.multiple_of(n * 256, 256), 256)
            both = jnp.dot(stack[...], c3[half, pl.ds(0, DEEP), at], preferred_element_type=F32)
            rest = jnp.dot(stack[pl.ds(0, rows), :], c3[half, pl.ds(2 * DEEP, DEEP), at], preferred_element_type=F32)
            to[:, at] = both[:rows] + both[rows:] + rest
            return 0

        lax.fori_loop(0, 2, body, 0)

    own_c.wait()
    split_c(0, core)
    own_h.wait()
    split_h(0, 0, 0, SLOT[0] * SUB)

    def along_x(dz, rows, swapped=False):
        r, l = rows[::-1] if swapped else rows, rows
        for a, b in zip(l, r):
            xs.setdefault(dz, []).extend(
                [send(hb.at[0, dz, a], hb.at[3, dz, a], xp), send(hb.at[0, dz, b], hb.at[1, dz, b], xm)]
            )

    xs = {}
    to_m["A"].wait_recv()
    along_x(1, [A])
    to_p["A"].wait_recv()
    along_x(3, [A])
    to_p["R"].wait_recv()
    far_p = send(rl.at[0], hb.at[0, 2, A], zp)
    to_m["R"].wait_recv()
    far_m = send(rl.at[1], hb.at[0, 2, B], zm)
    ca1.wait_recv()
    cc1 = send(cb.at[1, core, C1], cb.at[3, core, C1], yb)
    cb0.wait_recv()
    cc0 = send(cb.at[2, core, C0], cb.at[3, core, C0], ya)
    twins[1, 1] = send(cb.at[1, core, C1], cb.at[1, core, C1], twin)
    twins[2, 0] = send(cb.at[2, core, C0], cb.at[2, core, C0], twin)
    twins[0, 0].wait_recv()
    split_c(0, 1 - core)
    to_m["B"].wait_recv()
    along_x(1, [B])
    to_p["B"].wait_recv()
    along_x(3, [B])
    split_h(0, 1, 0, SLOT[1] * SUB)
    split_h(0, 3, 0, SLOT[3] * SUB)
    far_p.wait_recv()
    far_m.wait_recv()
    along_x(2, [A, B], swapped=True)
    ca0.wait_recv()
    twins[1, 0] = send(cb.at[1, core, C0], cb.at[1, core, C0], twin)
    cb1.wait_recv()
    twins[2, 1] = send(cb.at[2, core, C1], cb.at[2, core, C1], twin)
    split_h(0, 2, 0, SLOT[2] * SUB)
    split_c(1, core)
    twins[1, 1].wait_recv()
    twins[1, 0].wait_recv()
    split_c(1, 1 - core)

    def lies(group, dz, half, hs):
        if group == 1:
            return part.at[1 if dz in (1, 3) else 2, hs, pl.ds((128 if dz in (3, 0) else 0) + half * 64, 64), :]
        return part.at[0 if group == 0 else 3, hs, pl.ds(SLOT[dz] * 64 + half * 32, 32), :]

    def add(to, *terms):
        def body(i, _):
            at = pl.ds(pl.multiple_of(i * 8, 8), 8)
            total = terms[0][at, :]
            for term in terms[1:]:
                total = total + term[at, :]
            to[at, :] = total
            return 0

        lax.fori_loop(0, to.shape[0] // 8, body, 0)

    def add_to(to, box):
        for plane in range(to.shape[0]):
            add(to.at[plane], to.at[plane], box.at[plane])

    class Scatter:
        def __init__(self, group, box, hs):
            self.group, self.box, self.hs = group, box, hs

        def lie(self, dz, half):
            return lies(self.group, dz, half, self.hs)

        def far(self):
            self.p2 = send(self.lie(2, 0), self.box.at[0], zp)
            self.m2 = send(self.lie(2, 1), self.box.at[1], zm)

        def clean_p(self):
            self.cp = send(self.lie(1, 1), self.box.at[2], zp)

        def clean_m(self):
            self.cm = send(self.lie(3, 0), self.box.at[3], zm)

        def dirty_p(self):
            self.p2.wait_recv()
            add_to(self.lie(1, 0), self.box.at[0])
            self.dp = send(self.lie(1, 0), self.box.at[4], zp)

        def dirty_m(self):
            self.m2.wait_recv()
            add_to(self.lie(3, 1), self.box.at[1])
            self.dm = send(self.lie(3, 1), self.box.at[5], zm)

        def here(self):
            for copy in (self.cm, self.dp, self.cp, self.dm):
                copy.wait_recv()

    def rows_of(dx, first, rows):
        return pl.ds(pl.multiple_of((up(x, dx) * 2 + yh) * SUB + first, 8), rows)

    across = []

    def finish(half, terms, box, plane, dx, first, rows, side, at=0):
        came = [box.at[k, plane, pl.ds(at, rows)] for k in ((3, 4), (2, 5))[side]]
        where = rows_of(dx, first, rows)
        if half == 0:
            add(o_ref.at[where], terms, *came)
        else:
            add(terms, terms, *came)
            across.append(send(terms, o_ref.at[where], yc))

    near = [Scatter(0, r0.at[h], pl.ds(h, 1)) for h in range(2)]
    sides = [Scatter(1, r13.at[h], pl.ds(h, 1)) for h in range(2)]
    last = [Scatter(2, r2.at[h], pl.ds(h, 1)) for h in range(2)]

    multiply(0, 0, 0, 256)
    near[0].far()
    near[0].clean_p()
    near[0].clean_m()
    split_c(2, core)
    twins[2, 0].wait_recv()
    twins[2, 1].wait_recv()
    split_c(2, 1 - core)
    near[0].dirty_p()
    near[0].dirty_m()

    for dz, at in ((1, 0), (3, 128)):
        for copy in xs[dz]:
            copy.wait_recv()
        split_h(1, dz, 1, at)
        split_h(3, dz, 1, at + SUB)
    multiply(1, 0, 0, 256)
    sides[0].clean_p()
    sides[0].clean_m()
    cc1.wait_recv()
    twins[3, 1] = send(cb.at[3, core, C1], cb.at[3, core, C1], twin)
    cc0.wait_recv()
    twins[3, 0] = send(cb.at[3, core, C0], cb.at[3, core, C0], twin)
    split_c(3, core)
    twins[3, 1].wait_recv()
    twins[3, 0].wait_recv()
    split_c(3, 1 - core)

    multiply(0, 1, 0, 256)
    near[1].far()
    near[1].clean_p()
    near[1].clean_m()

    def onward(dz):
        return [send(hb.at[3, dz, A], hb.at[2, dz, A], xp), send(hb.at[1, dz, B], hb.at[2, dz, B], xm)]

    fs = {}
    for copy in xs[2][:2]:
        copy.wait_recv()
    for dz in (2, 1, 3):
        fs[dz] = onward(dz)
    for copy in x0:
        copy.wait_recv()
    fs[0] = onward(0)
    x1 = [send(hb.at[0, 0, p1], hb.at[3, 0, p1], xp), send(hb.at[0, 0, m1], hb.at[1, 0, m1], xm)]
    multiply(1, 1, 0, 256)
    sides[1].clean_p()
    sides[1].clean_m()
    near[1].dirty_p()
    near[1].dirty_m()
    for copy in xs[2][2:]:
        copy.wait_recv()
    split_h(1, 2, 2, 0)
    split_h(3, 2, 2, SUB)
    for h in (1, 0):
        multiply(2, h, 0, 128)
        sides[h].far()

    def opposite(dz):
        for copy in fs[dz]:
            copy.wait_recv()
        stack_h(2, dz, h2.at[dz], 0, SUB)

    def opposite_multiply(dz, h):
        multiply_stack(part.at[3, h, pl.ds(SLOT[dz] * 64, 64)], h2.at[dz], h)

    def finish_a(h):
        sides[h].here()
        finish(h, part.at[2, h, pl.ds(128, 48)], r13.at[h], 0, 1, 16, 48, 0, 16)
        finish(h, part.at[2, h, pl.ds(176, 48)], r13.at[h], 0, 3, 0, 48, 1, 0)

    def finish_b(h):
        multiply_stack(parts.at[h], hs, h)
        finish(h, parts.at[h, pl.ds(0, 16)], r13.at[h], 0, 1, 0, 16, 0, 0)
        finish(h, parts.at[h, pl.ds(16, 16)], r13.at[h], 0, 3, 48, 16, 1, 48)

    def finish_last(h):
        opposite_multiply(0, h)
        last[h].here()
        for side in range(2):
            finish(h, part.at[3, h, pl.ds(SLOT[0] * 64 + side * 32, 32)], r2.at[h], 0, 2, side * 32, 32, side)

    opposite(2)
    for h in (1, 0):
        opposite_multiply(2, h)
        last[h].far()
    for h in (1, 0):
        near[h].here()
        for side in range(2):
            finish(h, part.at[0, h, pl.ds(SLOT[0] * 64 + side * 32, 32)], r0.at[h], 0, 0, side * 32, 32, side)
    split_h(1, 0, 2, 128, 16, 48)
    split_h(3, 0, 2, 176, 0, 48)
    sides[1].dirty_p()
    sides[1].dirty_m()
    multiply(2, 1, 128, 96)
    sides[0].dirty_p()
    sides[0].dirty_m()
    opposite(1)
    for h in (1, 0):
        opposite_multiply(1, h)
        last[h].clean_p()
        last[h].dirty_p()
    finish_a(1)
    opposite(3)
    for h in (1, 0):
        opposite_multiply(3, h)
        last[h].clean_m()
        last[h].dirty_m()
    multiply(2, 0, 128, 96)
    finish_a(0)
    opposite(0)
    finish_last(1)
    for copy in x1:
        copy.wait_recv()
    stack_h(1, 0, hs, 0, 32, 0, 16)
    stack_h(3, 0, hs, 16, 32, 48, 16)
    finish_b(1)
    finish_last(0)
    finish_b(0)

    for copy in across:
        copy.wait_recv()
    for copy in sent:
        copy.wait_send()


def solution(mesh):
    def step(h, c):
        return pl.pallas_call(
            kernel,
            out_shape=pltpu.VMEM((512, WIDE), F32),
            in_specs=[pl.BlockSpec(memory_space=pl.ANY)] * 2,
            out_specs=pl.BlockSpec(memory_space=pltpu.VMEM),
            scratch_shapes=[
                pltpu.VMEM((4, 4, SUB, DEEP), F32),
                pltpu.VMEM((2, 32, DEEP), F32),
                pltpu.VMEM((4, 2, 512, WIDE), F32),
                pltpu.VMEM((2, 3 * DEEP, WIDE), BF16),
                pltpu.VMEM((3, 256, 3 * DEEP), BF16),
                pltpu.VMEM((4, 128, DEEP), BF16),
                pltpu.VMEM((64, DEEP), BF16),
                pltpu.VMEM((4, 2, 256, WIDE), F32),
                pltpu.VMEM((2, 32, WIDE), F32),
                pltpu.VMEM((2, 6, 1, 32, WIDE), F32),
                pltpu.VMEM((2, 6, 1, 64, WIDE), F32),
                pltpu.VMEM((2, 6, 1, 32, WIDE), F32),
                pltpu.SemaphoreType.DMA((96,)),
                pltpu.SemaphoreType.DMA((96,)),
                pltpu.SemaphoreType.DMA((2,)),
            ],
            compiler_params=pltpu.CompilerParams(collective_id=0, has_side_effects=True, vmem_limit_bytes=56 * 2**20),
        )(h, c)

    return jax.shard_map(
        step,
        mesh=mesh,
        in_specs=(P(("row", "col"), None), P("row", "col")),
        out_specs=P("row", "col"),
        check_vma=False,
    )
```

```python
import jax
import jax.numpy as jnp
from jax import lax
from jax.experimental import pallas as pl
from jax.experimental.pallas import tpu as pltpu
from jax.sharding import PartitionSpec as P

MESH = pl.DeviceIdType.MESH
F32, BF16 = jnp.float32, jnp.bfloat16
SUB = 64
DEEP = 2048
WIDE = 512
SLOT = {2: 0, 1: 1, 3: 2, 0: 3}
ROWS, ORBITALS, TWIN, SUMS, HALVES = range(5)
GROUPS = 46


def kernel(h_ref, c_ref, o_ref, hb, rl, cb, c3, h3, h2, ha, he, hz, part, pa, pe, pz, r0, r13, r2, ssem, rsem, lsem):
    row, col = lax.axis_index("row"), lax.axis_index("col")
    z, yl, core = lax.div(row, 4), lax.rem(lax.div(row, 2), 2), lax.rem(row, 2)
    x, yh = lax.div(col, 2), lax.rem(col, 2)

    def device(z=z, yl=yl, core=core, x=x, yh=yh):
        return ((z * 2 + yl) * 2 + core, x * 2 + yh)

    def up(v, d):
        return lax.rem(v + d, 4)

    zp, zm = device(z=up(z, 1)), device(z=up(z, 3))
    xp, xm = device(x=up(x, 1)), device(x=up(x, 3))
    ya, yb, yc = device(yl=1 - yl), device(yl=1 - yl, yh=1 - yh), device(yh=1 - yh)
    twin = device(core=1 - core)

    barrier = pltpu.get_barrier_semaphore()
    for other in (zp, zm, xp, xm, ya, yb, yc, twin):
        pl.semaphore_signal(barrier, inc=1, device_id=other, device_id_type=MESH)
    pl.semaphore_wait(barrier, 8)

    local, groups = [], []

    def group():
        groups.append(None)
        return rsem.at[len(groups) - 1]

    def send(src, dst, to, kind, into=None):
        copy = pltpu.make_async_remote_copy(
            src_ref=src,
            dst_ref=dst,
            send_sem=ssem.at[kind],
            recv_sem=group() if into is None else into,
            device_id=to,
            device_id_type=MESH,
        )
        copy.start()
        return copy

    def wait_for(like, sem):
        pltpu.make_async_copy(like, like, sem).wait()

    def move(src, dst):
        copy = pltpu.make_async_copy(src, dst, lsem.at[len(local)])
        copy.start()
        local.append(copy)
        return copy

    def inner(d):
        return pl.ds(pl.multiple_of(up(z, d) * DEEP, DEEP), DEEP)

    A, B, ALL = pl.ds(0, 32), pl.ds(32, 32), pl.ds(0, 64)
    C0, C1 = pl.ds(0, 256), pl.ds(256, 256)

    to_p, to_m = {}, {}
    own_h = move(h_ref.at[:, inner(0)], hb.at[0, 0])
    own_c = move(c_ref, cb.at[0, core])
    to_p["A"] = send(h_ref.at[A, inner(1)], hb.at[0, 3, A], zp, ROWS)
    to_m["A"] = send(h_ref.at[A, inner(3)], hb.at[0, 1, A], zm, ROWS)
    p0, m0 = pl.ds(0, 48), pl.ds(16, 48)
    x0 = group()
    send(h_ref.at[p0, inner(0)], hb.at[3, 0, p0], xp, ROWS, x0)
    send(h_ref.at[m0, inner(0)], hb.at[1, 0, m0], xm, ROWS, x0)
    ca1 = send(c_ref.at[C1], cb.at[1, core, C1], ya, ORBITALS)
    cb0 = send(c_ref.at[C0], cb.at[2, core, C0], yb, ORBITALS)
    to_p["R"] = send(h_ref.at[A, inner(2)], rl.at[0], zp, ROWS)
    to_m["R"] = send(h_ref.at[B, inner(2)], rl.at[1], zm, ROWS)
    ca0 = send(c_ref.at[C0], cb.at[1, core, C0], ya, ORBITALS)
    cb1 = send(c_ref.at[C1], cb.at[2, core, C1], yb, ORBITALS)
    to_p["B"] = send(h_ref.at[B, inner(1)], hb.at[0, 3, B], zp, ROWS)
    to_m["B"] = send(h_ref.at[B, inner(3)], hb.at[0, 1, B], zm, ROWS)
    own_twin = send(c_ref, cb.at[0, core], twin, TWIN)

    def split(src, rows, stores):
        def body(i, _):
            at = pl.multiple_of(i * 16, 16)
            v = src[pl.ds(at, 16), :]
            hi = v.astype(BF16)
            lo = (v - hi.astype(F32)).astype(BF16)
            for store in stores:
                store(at, hi, lo)
            return 0

        lax.fori_loop(0, rows // 16, body, 0)

    def split_h(dx, dz, batch, start, first=0, rows=SUB):
        def store(at, hi, lo):
            to = pl.ds(pl.multiple_of(start + at, 16), 16)
            h3[batch, to, pl.ds(0, DEEP)] = hi
            h3[batch, to, pl.ds(DEEP, DEEP)] = lo
            h3[batch, to, pl.ds(2 * DEEP, DEEP)] = hi

        split(hb.at[dx, dz, pl.ds(first, rows)], rows, [store])

    def stack_h(dx, dz, to, start, height, first=0, rows=SUB):
        def store(at, hi, lo):
            to[pl.ds(pl.multiple_of(start + at, 16), 16), :] = hi
            to[pl.ds(pl.multiple_of(start + height + at, 16), 16), :] = lo

        split(hb.at[dx, dz, pl.ds(first, rows)], rows, [store])

    def stack_pair(first, second, to, start, height):
        v = jnp.concatenate([first[...], second[...]], axis=0)
        hi = v.astype(BF16)
        to[pl.ds(start, 16), :] = hi
        to[pl.ds(start + height, 16), :] = (v - hi.astype(F32)).astype(BF16)

    def split_c(rel, which):
        half = 0 if rel < 2 else 1
        lower = yl if rel in (0, 3) else 1 - yl
        start = lower * 1024 + which * 512

        def store(at, hi, lo):
            to = pl.multiple_of(start + at, 16)
            c3[half, pl.ds(to, 16), :] = hi
            c3[half, pl.ds(to + DEEP, 16), :] = hi
            c3[half, pl.ds(to + 2 * DEEP, 16), :] = lo

        split(cb.at[rel, which], 512, [store])

    def multiply(batch, half, start, rows):
        def body(n, _):
            at = pl.ds(pl.multiple_of(n * 256, 256), 256)
            part[batch, half, pl.ds(start, rows), at] = jnp.dot(
                h3[batch, pl.ds(start, rows), :], c3[half, :, at], preferred_element_type=F32
            )
            return 0

        lax.fori_loop(0, 2, body, 0)

    def multiply_stack(to, stack, half, tiles=None):
        rows = to.shape[0]

        def body(n, _):
            at = pl.ds(pl.multiple_of(n * 256, 256), 256)
            both = jnp.dot(stack[...], c3[half, pl.ds(0, DEEP), at], preferred_element_type=F32)
            rest = jnp.dot(stack[pl.ds(0, rows), :], c3[half, pl.ds(2 * DEEP, DEEP), at], preferred_element_type=F32)
            to[:, at] = both[:rows] + both[rows:] + rest
            return 0

        if tiles is None:
            lax.fori_loop(0, 2, body, 0)
        else:
            body(tiles, 0)

    own_c.wait()
    split_c(0, core)
    own_h.wait()
    split_h(0, 0, 0, SLOT[0] * SUB)

    def along_x(dz, a, b, sem):
        send(hb.at[0, dz, a], hb.at[3, dz, a], xp, ROWS, sem)
        send(hb.at[0, dz, b], hb.at[1, dz, b], xm, ROWS, sem)

    xs = {dz: group() for dz in range(4)}
    twins = {rel: group() for rel in (1, 2, 3)}
    to_m["A"].wait_recv()
    along_x(1, A, A, xs[1])
    to_p["A"].wait_recv()
    along_x(3, A, A, xs[3])
    to_p["R"].wait_recv()
    far_p = send(rl.at[0], hb.at[0, 2, A], zp, ROWS)
    to_m["R"].wait_recv()
    far_m = send(rl.at[1], hb.at[0, 2, B], zm, ROWS)
    ca1.wait_recv()
    cc1 = send(cb.at[1, core, C1], cb.at[3, core, C1], yb, ORBITALS)
    cb0.wait_recv()
    cc0 = send(cb.at[2, core, C0], cb.at[3, core, C0], ya, ORBITALS)
    send(cb.at[1, core, C1], cb.at[1, core, C1], twin, TWIN, twins[1])
    send(cb.at[2, core, C0], cb.at[2, core, C0], twin, TWIN, twins[2])
    own_twin.wait_recv()
    split_c(0, 1 - core)
    to_m["B"].wait_recv()
    along_x(1, B, B, xs[1])
    to_p["B"].wait_recv()
    split_h(0, 1, 0, SLOT[1] * SUB)
    split_h(0, 3, 0, SLOT[3] * SUB)
    far_p.wait_recv()
    far_m.wait_recv()
    along_x(2, A, B, xs[0])
    along_x(2, B, A, xs[2])
    along_x(3, B, B, xs[3])
    ca0.wait_recv()
    send(cb.at[1, core, C0], cb.at[1, core, C0], twin, TWIN, twins[1])
    cb1.wait_recv()
    send(cb.at[2, core, C1], cb.at[2, core, C1], twin, TWIN, twins[2])
    split_h(0, 2, 0, SLOT[2] * SUB)
    split_c(1, core)
    wait_for(cb.at[0, 0], twins[1])
    split_c(1, 1 - core)

    def lies(group, dz, half, hs):
        if group == 1:
            return part.at[1 if dz in (1, 3) else 2, hs, pl.ds((128 if dz in (3, 0) else 0) + half * 64, 64), :]
        return part.at[0 if group == 0 else 3, hs, pl.ds(SLOT[dz] * 64 + half * 32, 32), :]

    def add(to, *terms):
        def body(i, _):
            at = pl.ds(pl.multiple_of(i * 8, 8), 8)
            total = terms[0][at, :]
            for term in terms[1:]:
                total = total + term[at, :]
            to[at, :] = total
            return 0

        lax.fori_loop(0, to.shape[0] // 8, body, 0)

    def add_to(to, box):
        for plane in range(to.shape[0]):
            add(to.at[plane], to.at[plane], box.at[plane])

    class Scatter:
        def __init__(self, which, box, hs):
            self.group, self.box, self.hs, self.sem = which, box, hs, group()

        def lie(self, dz, half):
            return lies(self.group, dz, half, self.hs)

        def far(self):
            self.p2 = send(self.lie(2, 0), self.box.at[0], zp, SUMS)
            self.m2 = send(self.lie(2, 1), self.box.at[1], zm, SUMS)

        def clean_p(self):
            send(self.lie(1, 1), self.box.at[2], zp, SUMS, self.sem)

        def clean_m(self):
            send(self.lie(3, 0), self.box.at[3], zm, SUMS, self.sem)

        def dirty_p(self):
            self.p2.wait_recv()
            add_to(self.lie(1, 0), self.box.at[0])
            send(self.lie(1, 0), self.box.at[4], zp, SUMS, self.sem)

        def dirty_m(self):
            self.m2.wait_recv()
            add_to(self.lie(3, 1), self.box.at[1])
            send(self.lie(3, 1), self.box.at[5], zm, SUMS, self.sem)

        def here(self):
            wait_for(part.at[0, 0, pl.ds(0, 4 * self.box.shape[2])], self.sem)

    class OneWay:
        def __init__(self, box, h):
            self.box, self.sem, self.at = box, group(), [part.at[3, h, pl.ds(SLOT[dz] * 64, 64)] for dz in range(4)]

        def far(self):
            self.f = send(self.at[2], self.box.at[0], zp, SUMS)

        def upper(self):
            self.f.wait_recv()
            add(self.at[1], self.at[1], self.box.at[0])
            send(self.at[1], self.box.at[1], zp, SUMS, self.sem)

        def lower(self):
            send(self.at[3], self.box.at[2], zm, SUMS, self.sem)

        def here(self):
            wait_for(part.at[0, 0, pl.ds(0, 128)], self.sem)

    def rows_of(dx, first, rows):
        return pl.ds(pl.multiple_of((up(x, dx) * 2 + yh) * SUB + first, 8), rows)

    across = group()

    def finish(half, terms, box, dx, first, rows, side, at=0, cols=pl.ds(0, WIDE)):
        planes = (3, 4), (2, 5)
        if side is None:
            came = [box.at[k, pl.ds(at, rows), cols] for k in (1, 2)]
        else:
            came = [box.at[k, 0, pl.ds(at, rows), cols] for k in planes[side]]
        where = rows_of(dx, first, rows)
        if half == 0:
            add(o_ref.at[where, cols], terms, *came)
        else:
            add(terms, terms, *came)
            send(terms, o_ref.at[where, cols], yc, HALVES, across)

    near = [Scatter(0, r0.at[h], pl.ds(h, 1)) for h in range(2)]
    sides = [Scatter(1, r13.at[h], pl.ds(h, 1)) for h in range(2)]
    last = [OneWay(r2.at[h], h) for h in range(2)]

    multiply(0, 0, 0, 256)
    near[0].far()
    near[0].clean_p()
    near[0].clean_m()
    split_c(2, core)
    wait_for(cb.at[0, 0], twins[2])
    split_c(2, 1 - core)
    near[0].dirty_p()
    near[0].dirty_m()

    def beside(dz, batch, start):
        wait_for(hb.at[0, 0] if dz == 2 else hb.at[pl.ds(0, 2), 0], xs[dz])
        split_h(1, dz, batch, start)
        split_h(3, dz, batch, start + SUB)

    beside(1, 1, 0)
    multiply(1, 0, 0, 128)
    sides[0].clean_p()
    cc1.wait_recv()
    send(cb.at[3, core, C1], cb.at[3, core, C1], twin, TWIN, twins[3])
    cc0.wait_recv()
    send(cb.at[3, core, C0], cb.at[3, core, C0], twin, TWIN, twins[3])
    split_c(3, core)
    wait_for(cb.at[0, 0], twins[3])
    split_c(3, 1 - core)

    multiply(0, 1, 0, 256)
    near[1].far()
    near[1].clean_p()
    near[1].clean_m()

    def onward(dz, a, b, sem):
        send(hb.at[3, dz, a], hb.at[2, dz, a], xp, ROWS, sem)
        send(hb.at[1, dz, b], hb.at[2, dz, b], xm, ROWS, sem)
        return sem

    fs = {}
    wait_for(hb.at[0, 0], xs[0])
    fs[2] = onward(2, A, B, group())
    fs[1] = onward(1, A, B, group())
    beside(2, 2, 0)
    multiply(2, 1, 0, 128)
    sides[1].far()
    multiply(1, 1, 0, 128)
    sides[1].clean_p()
    multiply(2, 0, 0, 128)
    near[1].dirty_p()
    near[1].dirty_m()
    beside(3, 1, 128)
    fs[3] = onward(3, A, B, group())
    wait_for(hb.at[pl.ds(0, 2), 0, pl.ds(0, 48)], x0)

    def rest(a, b, sem):
        send(hb.at[0, 0, a], hb.at[3, 0, a], xp, ROWS, sem)
        send(hb.at[0, 0, b], hb.at[1, 0, b], xm, ROWS, sem)

    early, late, end = group(), group(), group()
    rest(pl.ds(48, 8), pl.ds(8, 8), early)
    onward(0, pl.ds(0, 16), pl.ds(32, 16), early)
    onward(0, pl.ds(16, 16), pl.ds(48, 16), late)
    rest(pl.ds(56, 8), pl.ds(0, 8), end)
    multiply(1, 1, 128, 128)
    sides[1].clean_m()
    sides[1].dirty_p()
    sides[1].dirty_m()
    multiply(1, 0, 128, 128)
    split_h(1, 0, 2, 128, 16, 48)
    split_h(3, 0, 2, 176, 0, 48)
    multiply(2, 1, 128, 96)

    def opposite(dz):
        wait_for(hb.at[0, 0], fs[dz])
        stack_h(2, dz, h2.at[dz], 0, SUB)

    def opposite_multiply(dz, h):
        multiply_stack(part.at[3, h, pl.ds(SLOT[dz] * 64, 64)], h2.at[dz], h)

    def finish_a(h):
        sides[h].here()
        finish(h, part.at[2, h, pl.ds(128, 48)], r13.at[h], 1, 16, 48, 0, 16)
        finish(h, part.at[2, h, pl.ds(176, 48)], r13.at[h], 3, 0, 48, 1, 0)

    def finish_early(h):
        finish(h, pa.at[h, pl.ds(0, 16)], r2.at[h], 2, 0, 16, None, 0)
        finish(h, pa.at[h, pl.ds(16, 16)], r2.at[h], 2, 32, 16, None, 32)

    def finish_side(h):
        finish(h, pa.at[h, pl.ds(32, 8)], r13.at[h], 1, 8, 8, 0, 8)
        finish(h, pa.at[h, pl.ds(40, 8)], r13.at[h], 3, 48, 8, 1, 48)

    def finish_late(h):
        finish(h, pe.at[h, pl.ds(0, 16)], r2.at[h], 2, 16, 16, None, 16)
        finish(h, pe.at[h, pl.ds(16, 16)], r2.at[h], 2, 48, 16, None, 48)

    def finish_end(h, cols):
        finish(h, pz.at[h, pl.ds(0, 8), cols], r13.at[h], 1, 0, 8, 0, 0, cols)
        finish(h, pz.at[h, pl.ds(8, 8), cols], r13.at[h], 3, 56, 8, 1, 56, cols)

    opposite(2)
    opposite_multiply(2, 1)
    last[1].far()
    sides[0].far()
    sides[0].clean_m()
    opposite_multiply(2, 0)
    multiply(2, 0, 128, 96)
    opposite(1)
    opposite_multiply(1, 1)
    last[1].upper()
    last[0].far()
    finish_a(1)
    sides[0].dirty_m()
    opposite_multiply(1, 0)
    for h in (1, 0):
        near[h].here()
        for side in range(2):
            finish(h, part.at[0, h, pl.ds(SLOT[0] * 64 + side * 32, 32)], r0.at[h], 0, side * 32, 32, side)
    sides[0].dirty_p()
    opposite(3)
    opposite_multiply(3, 1)
    last[1].lower()
    opposite_multiply(3, 0)
    last[0].lower()
    wait_for(hb.at[0, 0, pl.ds(0, 48)], early)
    stack_h(2, 0, ha, 0, 48, 0, 16)
    stack_h(2, 0, ha, 16, 48, 32, 16)
    stack_pair(hb.at[1, 0, pl.ds(8, 8)], hb.at[3, 0, pl.ds(48, 8)], ha, 32, 48)
    multiply_stack(pa.at[1], ha, 1)
    finish_side(1)
    last[1].here()
    finish_early(1)
    last[0].upper()
    wait_for(hb.at[0, 0, pl.ds(0, 32)], late)
    stack_h(2, 0, he, 0, 32, 16, 16)
    stack_h(2, 0, he, 16, 32, 48, 16)
    multiply_stack(pe.at[1], he, 1)
    finish_late(1)
    wait_for(hb.at[0, 0, pl.ds(0, 16)], end)
    stack_pair(hb.at[1, 0, pl.ds(0, 8)], hb.at[3, 0, pl.ds(56, 8)], hz, 0, 16)
    for n in range(2):
        multiply_stack(pz.at[1], hz, 1, n)
        finish_end(1, pl.ds(n * 256, 256))
    multiply_stack(pa.at[0], ha, 0)
    multiply_stack(pe.at[0], he, 0)
    finish_a(0)
    finish_side(0)
    multiply_stack(pz.at[0], hz, 0)
    finish_end(0, pl.ds(0, WIDE))
    last[0].here()
    finish_early(0)
    finish_late(0)

    wait_for(hb, ssem.at[ROWS])
    wait_for(cb.at[pl.ds(0, 3), 0], ssem.at[ORBITALS])
    wait_for(cb.at[pl.ds(0, 4), 0], ssem.at[TWIN])
    wait_for(part.at[pl.ds(0, 3)], ssem.at[SUMS])
    wait_for(o_ref.at[pl.ds(0, 256)], ssem.at[HALVES])
    wait_for(o_ref.at[pl.ds(0, 256)], across)


def solution(mesh):
    def step(h, c):
        return pl.pallas_call(
            kernel,
            out_shape=pltpu.VMEM((512, WIDE), F32),
            in_specs=[pl.BlockSpec(memory_space=pl.ANY)] * 2,
            out_specs=pl.BlockSpec(memory_space=pltpu.VMEM),
            scratch_shapes=[
                pltpu.VMEM((4, 4, SUB, DEEP), F32),
                pltpu.VMEM((2, 32, DEEP), F32),
                pltpu.VMEM((4, 2, 512, WIDE), F32),
                pltpu.VMEM((2, 3 * DEEP, WIDE), BF16),
                pltpu.VMEM((3, 256, 3 * DEEP), BF16),
                pltpu.VMEM((4, 128, DEEP), BF16),
                pltpu.VMEM((96, DEEP), BF16),
                pltpu.VMEM((64, DEEP), BF16),
                pltpu.VMEM((32, DEEP), BF16),
                pltpu.VMEM((4, 2, 256, WIDE), F32),
                pltpu.VMEM((2, 48, WIDE), F32),
                pltpu.VMEM((2, 32, WIDE), F32),
                pltpu.VMEM((2, 16, WIDE), F32),
                pltpu.VMEM((2, 6, 1, 32, WIDE), F32),
                pltpu.VMEM((2, 6, 1, 64, WIDE), F32),
                pltpu.VMEM((2, 3, 64, WIDE), F32),
                pltpu.SemaphoreType.DMA((5,)),
                pltpu.SemaphoreType.DMA((GROUPS,)),
                pltpu.SemaphoreType.DMA((2,)),
            ],
            compiler_params=pltpu.CompilerParams(collective_id=0, has_side_effects=True, vmem_limit_bytes=56 * 2**20),
        )(h, c)

    return jax.shard_map(
        step,
        mesh=mesh,
        in_specs=(P(("row", "col"), None), P("row", "col")),
        out_specs=P("row", "col"),
        check_vma=False,
    )
```

```python
import jax
import jax.numpy as jnp
from jax import lax
from jax.experimental import pallas as pl
from jax.experimental.pallas import tpu as pltpu
from jax.sharding import PartitionSpec as P

MESH = pl.DeviceIdType.MESH
F32, BF16 = jnp.float32, jnp.bfloat16
SUB = 64
DEEP = 2048
WIDE = 512
SLOT = {2: 0, 1: 1, 3: 2, 0: 3}
ROWS, ORBITALS, TWIN, SUMS, HALVES = range(5)
GROUPS = 46


def kernel(h_ref, c_ref, o_ref, hb, rl, cb, c3, h3, h2, ha, he, hz, part, pa, pe, pz, r0, r13, r2, ssem, rsem, lsem):
    row, col = lax.axis_index("row"), lax.axis_index("col")
    z, yl, core = lax.div(row, 4), lax.rem(lax.div(row, 2), 2), lax.rem(row, 2)
    x, yh = lax.div(col, 2), lax.rem(col, 2)

    def device(z=z, yl=yl, core=core, x=x, yh=yh):
        return ((z * 2 + yl) * 2 + core, x * 2 + yh)

    def up(v, d):
        return lax.rem(v + d, 4)

    zp, zm = device(z=up(z, 1)), device(z=up(z, 3))
    xp, xm = device(x=up(x, 1)), device(x=up(x, 3))
    ya, yb, yc = device(yl=1 - yl), device(yl=1 - yl, yh=1 - yh), device(yh=1 - yh)
    twin = device(core=1 - core)

    barrier = pltpu.get_barrier_semaphore()
    for other in (zp, zm, xp, xm, ya, yb, yc, twin):
        pl.semaphore_signal(barrier, inc=1, device_id=other, device_id_type=MESH)
    pl.semaphore_wait(barrier, 8)

    local, groups = [], []

    def group():
        groups.append(None)
        return rsem.at[len(groups) - 1]

    def send(src, dst, to, kind, into=None):
        copy = pltpu.make_async_remote_copy(
            src_ref=src,
            dst_ref=dst,
            send_sem=ssem.at[kind],
            recv_sem=group() if into is None else into,
            device_id=to,
            device_id_type=MESH,
        )
        copy.start()
        return copy

    def wait_for(like, sem):
        pltpu.make_async_copy(like, like, sem).wait()

    def move(src, dst):
        copy = pltpu.make_async_copy(src, dst, lsem.at[len(local)])
        copy.start()
        local.append(copy)
        return copy

    def inner(d):
        return pl.ds(pl.multiple_of(up(z, d) * DEEP, DEEP), DEEP)

    A, B, ALL = pl.ds(0, 32), pl.ds(32, 32), pl.ds(0, 64)
    C0, C1 = pl.ds(0, 256), pl.ds(256, 256)

    to_p, to_m = {}, {}
    own_h = move(h_ref.at[:, inner(0)], hb.at[0, 0])
    own_c = move(c_ref, cb.at[0, core])
    to_p["A"] = send(h_ref.at[A, inner(1)], hb.at[0, 3, A], zp, ROWS)
    to_m["A"] = send(h_ref.at[A, inner(3)], hb.at[0, 1, A], zm, ROWS)
    p0, m0 = pl.ds(0, 48), pl.ds(16, 48)
    x0 = group()
    send(h_ref.at[p0, inner(0)], hb.at[3, 0, p0], xp, ROWS, x0)
    send(h_ref.at[m0, inner(0)], hb.at[1, 0, m0], xm, ROWS, x0)
    ca1 = send(c_ref.at[C1], cb.at[1, core, C1], ya, ORBITALS)
    cb0 = send(c_ref.at[C0], cb.at[2, core, C0], yb, ORBITALS)
    to_p["R"] = send(h_ref.at[A, inner(2)], rl.at[0], zp, ROWS)
    to_m["R"] = send(h_ref.at[B, inner(2)], rl.at[1], zm, ROWS)
    ca0 = send(c_ref.at[C0], cb.at[1, core, C0], ya, ORBITALS)
    cb1 = send(c_ref.at[C1], cb.at[2, core, C1], yb, ORBITALS)
    to_p["B"] = send(h_ref.at[B, inner(1)], hb.at[0, 3, B], zp, ROWS)
    to_m["B"] = send(h_ref.at[B, inner(3)], hb.at[0, 1, B], zm, ROWS)
    own_twin = send(c_ref, cb.at[0, core], twin, TWIN)

    def split(src, rows, stores):
        def body(i, _):
            at = pl.multiple_of(i * 16, 16)
            v = src[pl.ds(at, 16), :]
            hi = v.astype(BF16)
            lo = (v - hi.astype(F32)).astype(BF16)
            for store in stores:
                store(at, hi, lo)
            return 0

        lax.fori_loop(0, rows // 16, body, 0)

    def split_h(dx, dz, batch, start, first=0, rows=SUB):
        def store(at, hi, lo):
            to = pl.ds(pl.multiple_of(start + at, 16), 16)
            h3[batch, to, pl.ds(0, DEEP)] = hi
            h3[batch, to, pl.ds(DEEP, DEEP)] = lo
            h3[batch, to, pl.ds(2 * DEEP, DEEP)] = hi

        split(hb.at[dx, dz, pl.ds(first, rows)], rows, [store])

    def stack_h(dx, dz, to, start, height, first=0, rows=SUB):
        def store(at, hi, lo):
            to[pl.ds(pl.multiple_of(start + at, 16), 16), :] = hi
            to[pl.ds(pl.multiple_of(start + height + at, 16), 16), :] = lo

        split(hb.at[dx, dz, pl.ds(first, rows)], rows, [store])

    def stack_pair(first, second, to, start, height):
        v = jnp.concatenate([first[...], second[...]], axis=0)
        hi = v.astype(BF16)
        to[pl.ds(start, 16), :] = hi
        to[pl.ds(start + height, 16), :] = (v - hi.astype(F32)).astype(BF16)

    def split_c(rel, which):
        half = 0 if rel < 2 else 1
        lower = yl if rel in (0, 3) else 1 - yl
        start = lower * 1024 + which * 512

        def store(at, hi, lo):
            to = pl.multiple_of(start + at, 16)
            c3[half, pl.ds(to, 16), :] = hi
            c3[half, pl.ds(to + DEEP, 16), :] = hi
            c3[half, pl.ds(to + 2 * DEEP, 16), :] = lo

        split(cb.at[rel, which], 512, [store])

    def multiply(batch, half, start, rows):
        def body(n, _):
            at = pl.ds(pl.multiple_of(n * 256, 256), 256)
            part[batch, half, pl.ds(start, rows), at] = jnp.dot(
                h3[batch, pl.ds(start, rows), :], c3[half, :, at], preferred_element_type=F32
            )
            return 0

        lax.fori_loop(0, 2, body, 0)

    def multiply_stack(to, stack, half, tile=None):
        rows = to.shape[0]

        at = pl.ds(0, WIDE) if tile is None else pl.ds(tile * 256, 256)
        both = jnp.dot(stack[...], c3[half, pl.ds(0, DEEP), at], preferred_element_type=F32)
        rest = jnp.dot(stack[pl.ds(0, rows), :], c3[half, pl.ds(2 * DEEP, DEEP), at], preferred_element_type=F32)
        to[:, at] = both[:rows] + both[rows:] + rest

    own_c.wait()
    split_c(0, core)
    own_h.wait()
    split_h(0, 0, 0, SLOT[0] * SUB)

    def along_x(dz, a, b, sem):
        send(hb.at[0, dz, a], hb.at[3, dz, a], xp, ROWS, sem)
        send(hb.at[0, dz, b], hb.at[1, dz, b], xm, ROWS, sem)

    xs = {dz: group() for dz in range(4)}
    twins = {rel: group() for rel in (1, 2, 3)}
    to_m["A"].wait_recv()
    along_x(1, A, A, xs[1])
    to_p["A"].wait_recv()
    along_x(3, A, A, xs[3])
    to_p["R"].wait_recv()
    far_p = send(rl.at[0], hb.at[0, 2, A], zp, ROWS)
    to_m["R"].wait_recv()
    far_m = send(rl.at[1], hb.at[0, 2, B], zm, ROWS)
    ca1.wait_recv()
    cc1 = send(cb.at[1, core, C1], cb.at[3, core, C1], yb, ORBITALS)
    cb0.wait_recv()
    cc0 = send(cb.at[2, core, C0], cb.at[3, core, C0], ya, ORBITALS)
    send(cb.at[1, core, C1], cb.at[1, core, C1], twin, TWIN, twins[1])
    send(cb.at[2, core, C0], cb.at[2, core, C0], twin, TWIN, twins[2])
    own_twin.wait_recv()
    split_c(0, 1 - core)
    to_m["B"].wait_recv()
    along_x(1, B, B, xs[1])
    to_p["B"].wait_recv()
    split_h(0, 1, 0, SLOT[1] * SUB)
    split_h(0, 3, 0, SLOT[3] * SUB)
    far_p.wait_recv()
    far_m.wait_recv()
    along_x(2, A, B, xs[0])
    along_x(2, B, A, xs[2])
    along_x(3, B, B, xs[3])
    ca0.wait_recv()
    send(cb.at[1, core, C0], cb.at[1, core, C0], twin, TWIN, twins[1])
    cb1.wait_recv()
    send(cb.at[2, core, C1], cb.at[2, core, C1], twin, TWIN, twins[2])
    split_h(0, 2, 0, SLOT[2] * SUB)
    split_c(1, core)
    wait_for(cb.at[0, 0], twins[1])
    split_c(1, 1 - core)

    def lies(group, dz, half, hs):
        if group == 1:
            return part.at[1 if dz in (1, 3) else 2, hs, pl.ds((128 if dz in (3, 0) else 0) + half * 64, 64), :]
        return part.at[0 if group == 0 else 3, hs, pl.ds(SLOT[dz] * 64 + half * 32, 32), :]

    def add(to, *terms):
        def body(i, _):
            at = pl.ds(pl.multiple_of(i * 8, 8), 8)
            total = terms[0][at, :]
            for term in terms[1:]:
                total = total + term[at, :]
            to[at, :] = total
            return 0

        lax.fori_loop(0, to.shape[0] // 8, body, 0)

    def add_to(to, box):
        for plane in range(to.shape[0]):
            add(to.at[plane], to.at[plane], box.at[plane])

    class Scatter:
        def __init__(self, which, box, hs):
            self.group, self.box, self.hs, self.sem = which, box, hs, group()

        def lie(self, dz, half):
            return lies(self.group, dz, half, self.hs)

        def far(self):
            self.p2 = send(self.lie(2, 0), self.box.at[0], zp, SUMS)
            self.m2 = send(self.lie(2, 1), self.box.at[1], zm, SUMS)

        def clean_p(self):
            send(self.lie(1, 1), self.box.at[2], zp, SUMS, self.sem)

        def clean_m(self):
            send(self.lie(3, 0), self.box.at[3], zm, SUMS, self.sem)

        def dirty_p(self):
            self.p2.wait_recv()
            add_to(self.lie(1, 0), self.box.at[0])
            send(self.lie(1, 0), self.box.at[4], zp, SUMS, self.sem)

        def dirty_m(self):
            self.m2.wait_recv()
            add_to(self.lie(3, 1), self.box.at[1])
            send(self.lie(3, 1), self.box.at[5], zm, SUMS, self.sem)

        def here(self):
            wait_for(part.at[0, 0, pl.ds(0, 4 * self.box.shape[2])], self.sem)

    class OneWay:
        def __init__(self, box, h):
            self.box, self.sem, self.at = box, group(), [part.at[3, h, pl.ds(SLOT[dz] * 64, 64)] for dz in range(4)]

        def far(self):
            self.f = send(self.at[2], self.box.at[0], zp, SUMS)

        def upper(self):
            self.f.wait_recv()
            add(self.at[1], self.at[1], self.box.at[0])
            send(self.at[1], self.box.at[1], zp, SUMS, self.sem)

        def lower(self):
            send(self.at[3], self.box.at[2], zm, SUMS, self.sem)

        def here(self):
            wait_for(part.at[0, 0, pl.ds(0, 128)], self.sem)

    def rows_of(dx, first, rows):
        return pl.ds(pl.multiple_of((up(x, dx) * 2 + yh) * SUB + first, 8), rows)

    across = group()

    def finish(half, terms, box, dx, first, rows, side, at=0, cols=pl.ds(0, WIDE)):
        planes = (3, 4), (2, 5)
        if side is None:
            came = [box.at[k, pl.ds(at, rows), cols] for k in (1, 2)]
        else:
            came = [box.at[k, 0, pl.ds(at, rows), cols] for k in planes[side]]
        where = rows_of(dx, first, rows)
        if half == 0:
            add(o_ref.at[where, cols], terms, *came)
        else:
            add(terms, terms, *came)
            send(terms, o_ref.at[where, cols], yc, HALVES, across)

    near = [Scatter(0, r0.at[h], pl.ds(h, 1)) for h in range(2)]
    sides = [Scatter(1, r13.at[h], pl.ds(h, 1)) for h in range(2)]
    last = [OneWay(r2.at[h], h) for h in range(2)]

    multiply(0, 0, 0, 256)
    near[0].far()
    near[0].clean_p()
    near[0].clean_m()
    split_c(2, core)
    wait_for(cb.at[0, 0], twins[2])
    split_c(2, 1 - core)
    near[0].dirty_p()
    near[0].dirty_m()

    def beside(dz, batch, start):
        wait_for(hb.at[0, 0] if dz == 2 else hb.at[pl.ds(0, 2), 0], xs[dz])
        split_h(1, dz, batch, start)
        split_h(3, dz, batch, start + SUB)

    beside(1, 1, 0)
    multiply(1, 0, 0, 128)
    sides[0].clean_p()
    cc1.wait_recv()
    send(cb.at[3, core, C1], cb.at[3, core, C1], twin, TWIN, twins[3])
    cc0.wait_recv()
    send(cb.at[3, core, C0], cb.at[3, core, C0], twin, TWIN, twins[3])
    split_c(3, core)
    wait_for(cb.at[0, 0], twins[3])
    split_c(3, 1 - core)

    multiply(0, 1, 0, 256)
    near[1].far()
    near[1].clean_p()
    near[1].clean_m()

    def onward(dz, a, b, sem):
        send(hb.at[3, dz, a], hb.at[2, dz, a], xp, ROWS, sem)
        send(hb.at[1, dz, b], hb.at[2, dz, b], xm, ROWS, sem)
        return sem

    fs = {}
    wait_for(hb.at[0, 0], xs[0])
    fs[2] = onward(2, A, B, group())
    fs[1] = onward(1, A, B, group())
    beside(2, 2, 0)
    multiply(2, 1, 0, 128)
    sides[1].far()
    multiply(1, 1, 0, 128)
    sides[1].clean_p()
    multiply(2, 0, 0, 128)
    near[1].dirty_p()
    near[1].dirty_m()
    beside(3, 1, 128)
    fs[3] = onward(3, A, B, group())
    wait_for(hb.at[pl.ds(0, 2), 0, pl.ds(0, 48)], x0)

    def rest(a, b, sem):
        send(hb.at[0, 0, a], hb.at[3, 0, a], xp, ROWS, sem)
        send(hb.at[0, 0, b], hb.at[1, 0, b], xm, ROWS, sem)

    early, late, end = group(), group(), group()
    rest(pl.ds(48, 8), pl.ds(8, 8), early)
    onward(0, pl.ds(0, 16), pl.ds(32, 16), early)
    onward(0, pl.ds(16, 16), pl.ds(48, 16), late)
    rest(pl.ds(56, 8), pl.ds(0, 8), end)
    multiply(1, 1, 128, 128)
    sides[1].clean_m()
    sides[1].dirty_p()
    sides[1].dirty_m()
    multiply(1, 0, 128, 128)
    split_h(1, 0, 2, 128, 16, 48)
    split_h(3, 0, 2, 176, 0, 48)
    multiply(2, 1, 128, 96)

    def opposite(dz):
        wait_for(hb.at[0, 0], fs[dz])
        stack_h(2, dz, h2.at[dz], 0, SUB)

    def opposite_multiply(dz, h):
        multiply_stack(part.at[3, h, pl.ds(SLOT[dz] * 64, 64)], h2.at[dz], h)

    def finish_a(h):
        sides[h].here()
        finish(h, part.at[2, h, pl.ds(128, 48)], r13.at[h], 1, 16, 48, 0, 16)
        finish(h, part.at[2, h, pl.ds(176, 48)], r13.at[h], 3, 0, 48, 1, 0)

    def finish_early(h):
        finish(h, pa.at[h, pl.ds(0, 16)], r2.at[h], 2, 0, 16, None, 0)
        finish(h, pa.at[h, pl.ds(16, 16)], r2.at[h], 2, 32, 16, None, 32)

    def finish_side(h):
        finish(h, pa.at[h, pl.ds(32, 8)], r13.at[h], 1, 8, 8, 0, 8)
        finish(h, pa.at[h, pl.ds(40, 8)], r13.at[h], 3, 48, 8, 1, 48)

    def finish_late(h):
        finish(h, pe.at[h, pl.ds(0, 16)], r2.at[h], 2, 16, 16, None, 16)
        finish(h, pe.at[h, pl.ds(16, 16)], r2.at[h], 2, 48, 16, None, 48)

    def finish_end(h, cols):
        finish(h, pz.at[h, pl.ds(0, 8), cols], r13.at[h], 1, 0, 8, 0, 0, cols)
        finish(h, pz.at[h, pl.ds(8, 8), cols], r13.at[h], 3, 56, 8, 1, 56, cols)

    opposite(2)
    opposite_multiply(2, 1)
    last[1].far()
    sides[0].far()
    sides[0].clean_m()
    opposite_multiply(2, 0)
    multiply(2, 0, 128, 96)
    opposite(1)
    opposite_multiply(1, 1)
    last[1].upper()
    last[0].far()
    finish_a(1)
    sides[0].dirty_m()
    opposite_multiply(1, 0)
    for h in (1, 0):
        near[h].here()
        for side in range(2):
            finish(h, part.at[0, h, pl.ds(SLOT[0] * 64 + side * 32, 32)], r0.at[h], 0, side * 32, 32, side)
    sides[0].dirty_p()
    opposite(3)
    opposite_multiply(3, 1)
    last[1].lower()
    opposite_multiply(3, 0)
    last[0].lower()
    wait_for(hb.at[0, 0, pl.ds(0, 48)], early)
    stack_h(2, 0, ha, 0, 48, 0, 16)
    stack_h(2, 0, ha, 16, 48, 32, 16)
    stack_pair(hb.at[1, 0, pl.ds(8, 8)], hb.at[3, 0, pl.ds(48, 8)], ha, 32, 48)
    multiply_stack(pa.at[1], ha, 1)
    finish_side(1)
    last[1].here()
    finish_early(1)
    last[0].upper()
    wait_for(hb.at[0, 0, pl.ds(0, 32)], late)
    stack_h(2, 0, he, 0, 32, 16, 16)
    stack_h(2, 0, he, 16, 32, 48, 16)
    multiply_stack(pe.at[1], he, 1)
    finish_late(1)
    wait_for(hb.at[0, 0, pl.ds(0, 16)], end)
    stack_pair(hb.at[1, 0, pl.ds(0, 8)], hb.at[3, 0, pl.ds(56, 8)], hz, 0, 16)
    for n in range(2):
        multiply_stack(pz.at[1], hz, 1, n)
        finish_end(1, pl.ds(n * 256, 256))
    multiply_stack(pa.at[0], ha, 0)
    multiply_stack(pe.at[0], he, 0)
    finish_a(0)
    finish_side(0)
    multiply_stack(pz.at[0], hz, 0)
    finish_end(0, pl.ds(0, WIDE))
    last[0].here()
    finish_early(0)
    finish_late(0)

    wait_for(hb, ssem.at[ROWS])
    wait_for(cb.at[pl.ds(0, 3), 0], ssem.at[ORBITALS])
    wait_for(cb.at[pl.ds(0, 4), 0], ssem.at[TWIN])
    wait_for(part.at[pl.ds(0, 3)], ssem.at[SUMS])
    wait_for(o_ref.at[pl.ds(0, 256)], ssem.at[HALVES])
    wait_for(o_ref.at[pl.ds(0, 256)], across)


def solution(mesh):
    def step(h, c):
        return pl.pallas_call(
            kernel,
            out_shape=pltpu.VMEM((512, WIDE), F32),
            in_specs=[pl.BlockSpec(memory_space=pl.ANY)] * 2,
            out_specs=pl.BlockSpec(memory_space=pltpu.VMEM),
            scratch_shapes=[
                pltpu.VMEM((4, 4, SUB, DEEP), F32),
                pltpu.VMEM((2, 32, DEEP), F32),
                pltpu.VMEM((4, 2, 512, WIDE), F32),
                pltpu.VMEM((2, 3 * DEEP, WIDE), BF16),
                pltpu.VMEM((3, 256, 3 * DEEP), BF16),
                pltpu.VMEM((4, 128, DEEP), BF16),
                pltpu.VMEM((96, DEEP), BF16),
                pltpu.VMEM((64, DEEP), BF16),
                pltpu.VMEM((32, DEEP), BF16),
                pltpu.VMEM((4, 2, 256, WIDE), F32),
                pltpu.VMEM((2, 48, WIDE), F32),
                pltpu.VMEM((2, 32, WIDE), F32),
                pltpu.VMEM((2, 16, WIDE), F32),
                pltpu.VMEM((2, 6, 1, 32, WIDE), F32),
                pltpu.VMEM((2, 6, 1, 64, WIDE), F32),
                pltpu.VMEM((2, 3, 64, WIDE), F32),
                pltpu.SemaphoreType.DMA((5,)),
                pltpu.SemaphoreType.DMA((GROUPS,)),
                pltpu.SemaphoreType.DMA((2,)),
            ],
            compiler_params=pltpu.CompilerParams(collective_id=0, has_side_effects=True, vmem_limit_bytes=56 * 2**20),
        )(h, c)

    return jax.shard_map(
        step,
        mesh=mesh,
        in_specs=(P(("row", "col"), None), P("row", "col")),
        out_specs=P("row", "col"),
        check_vma=False,
    )
```
